32 devices in a mesh: panels: 32 (over z, y, x, core).
Axes of the slice: x: 2, y: 2, z: 4, core: 2. Of those that a mesh axis runs over, the one named last changes fastest.
Arguments:
- excitation: bfloat16 [64, 131072], P(None, 'panels'), may hold values from -6 to 6
- near_tiles: bfloat16 [512, 5, 256, 256], P('panels'), may hold values from -0.15625 to 0.15625
- near_offset: int32 [512, 5], P('panels'), may hold values from -16 to 16, as said below
- near_count: int32 [512], P('panels'), may hold values from 1 to 5, as said below
- far_src: int32 [32, 16], replicated, may hold values from 0 to 31, as said below
- far_count: int32 [32], replicated, may hold values from 1 to 16
- source_factor: bfloat16 [16, 32, 131072], P(None, None, 'panels'), may hold values from -0.09375 to 0.09375
- target_factor: bfloat16 [16, 32, 131072], P(None, None, 'panels'), may hold values from -0.25 to 0.25
Outputs:
- krylov: float32 [5, 64, 131072], P(None, None, 'panels')
The draws below stay inside these ranges and needn't reach their ends.
Inputs may be any that keep to these rules, and one draw needn't show every extreme that they name: `near_offset`: offsets within one leaf are distinct. `near_count`: some leaf has 5 live slots. `far_src`: within a row the entries are distinct and never the row itself. Counting live slots only, every block row is the source of at most 16 far blocks, and some block row of exactly 16.
All inputs are finite; a program needn't handle non-finite values.
Results may differ from the reference program's by a relative error of at most 0.0095.
Values may be sent and summed in bfloat16 or wider, within the bound.
A program may use at most 128 MiB of HBM per device.

```python
import jax
import jax.numpy as jnp
from jax import lax

LEAF = 256
EXCITE = 64
RANK = 32
NEAR = 5
FAR = 16
ITERS = 5
LEAVES_DEV = 16
PANELS_DEV = 4096
LEAVES = 512
PANELS = 131072
DEVS = 32


def draw_near_offset(key, part):
    choices_total = 2 * LEAVES_DEV + 1
    scores = jax.random.randint(key, (LEAVES, choices_total), 0, 1 << 20) * 128
    scores = scores + jnp.arange(choices_total, dtype=jnp.int32)[None, :]
    order = jnp.argsort(scores, axis=1)
    return (order[:, :NEAR] - LEAVES_DEV).astype(jnp.int32)


def draw_near_count(key, part):
    first_key, second_key = jax.random.split(key)
    counts = jax.random.randint(first_key, (LEAVES,), 1, NEAR + 1)
    pivot = jax.random.randint(second_key, (), 0, LEAVES)
    return counts.at[pivot].set(NEAR).astype(jnp.int32)


def far_plan(key):
    base = jax.random.fold_in(key, 7)
    perm_key, offset_key, slot_key, pivot_key = jax.random.split(base, 4)
    order = jax.random.permutation(perm_key, DEVS).astype(jnp.int32)
    inverse = jnp.zeros((DEVS,), jnp.int32).at[order].set(jnp.arange(DEVS, dtype=jnp.int32))
    offset_scores = jax.random.randint(offset_key, (DEVS - 1,), 0, 1 << 16) * DEVS
    offset_scores = offset_scores + jnp.arange(DEVS - 1, dtype=jnp.int32)
    offsets = (jnp.argsort(offset_scores)[:FAR] + 1).astype(jnp.int32)
    slot_scores = jax.random.randint(slot_key, (DEVS, FAR), 0, 1 << 16) * FAR
    slot_scores = slot_scores + jnp.arange(FAR, dtype=jnp.int32)[None, :]
    slot_order = jnp.argsort(slot_scores, axis=1).astype(jnp.int32)
    shifts = jnp.take(offsets, slot_order)
    far_src = jnp.take(inverse, (order[:, None] + shifts) % DEVS)
    pivot = jax.random.randint(pivot_key, (), 0, DEVS)
    full_rows = jnp.take(inverse, (order[pivot] - offsets) % DEVS)
    return (far_src.astype(jnp.int32), full_rows.astype(jnp.int32))


def draw_far_src(key, part):
    far_src, full_rows = far_plan(key)
    return far_src


def draw_far_count(key, part):
    far_src, full_rows = far_plan(key)
    own = jax.random.fold_in(key, 11)
    first_key, second_key = jax.random.split(own)
    left = jax.random.randint(first_key, (DEVS,), 0, FAR + 1)
    right = jax.random.randint(second_key, (DEVS,), 0, FAR + 1)
    counts = jnp.clip(1 + left * right // FAR, 1, FAR)
    return counts.at[full_rows].set(FAR).astype(jnp.int32)


def level_of(own_key, dims, pieces, low, high):
    factor_of, own = 1.0, jax.random.fold_in(own_key, 6)
    for axis_at, blocks in pieces:
        heights = jnp.exp(jax.random.uniform(jax.random.fold_in(own, axis_at), (blocks,), jnp.float32, low / len(pieces), high / len(pieces)))
        factor_of = factor_of * jnp.repeat(heights, dims[axis_at] // blocks).reshape([-1 if axis == axis_at else 1 for axis in range(len(dims))])
    return factor_of


def bell_draw(rng, dims, width, bound, shards=(), kind=jnp.bfloat16):
    values = width * jax.random.normal(rng, dims, jnp.float32)
    if shards:
        values = values * level_of(rng, dims, shards, -0.22, 0.18)
    return jnp.clip(values, -bound, bound).astype(kind)


def setup_inputs(seed: int = 0) -> dict:
    splits = jax.random.split(jax.random.key(seed), 9)
    excitation = bell_draw(splits[0], (EXCITE, PANELS), 1.0, 6.0, ((1, 32),))
    near_tiles = bell_draw(splits[1], (LEAVES, NEAR, LEAF, LEAF), (NEAR * LEAF) ** -0.5, 0.15625, ((0, 32),))
    near_offset = draw_near_offset(jax.random.fold_in(splits[8], 71), 0)
    near_count = draw_near_count(jax.random.fold_in(splits[8], 71), 0)
    far_src = draw_far_src(jax.random.fold_in(splits[8], 71), 0)
    far_count = draw_far_count(jax.random.fold_in(splits[8], 71), 0)
    source_factor = bell_draw(splits[6], (FAR, RANK, PANELS), PANELS_DEV ** -0.5, 0.09375, ((2, 32),))
    target_factor = bell_draw(splits[7], (FAR, RANK, PANELS), (RANK * FAR) ** -0.5, 0.25, ((2, 32),))
    return dict(excitation=excitation, near_tiles=near_tiles, near_offset=near_offset, near_count=near_count, far_src=far_src, far_count=far_count, source_factor=source_factor, target_factor=target_factor)


def out_ranks(far_src, far_count):
    row_total, slot_count = far_src.shape
    live_far = jnp.arange(slot_count, dtype=jnp.int32)[None, :] < far_count[:, None]
    owners = jnp.arange(row_total, dtype=jnp.int32)
    hits = ((far_src.reshape(-1)[:, None] == owners[None, :]) & live_far.reshape(-1)[:, None]).astype(jnp.int32)
    earlier = jnp.cumsum(hits, axis=0) - hits
    out_rank = jnp.sum(earlier * hits, axis=1).astype(jnp.int32)
    return out_rank.reshape(row_total, slot_count), live_far


def apply_operator(field, near_tiles, near_offset, near_count, far_src, out_rank, live_far, source_factor, target_factor):
    row_total = far_src.shape[0]
    leaf_total = near_tiles.shape[0]
    near_slots = near_tiles.shape[1]
    leaf_size = near_tiles.shape[2]
    leaves_local = leaf_total // row_total
    panels_local = leaves_local * leaf_size
    excite = field.shape[0]
    highest = lax.Precision.HIGHEST

    def coefficients(device):
        first = device * panels_local
        factor = lax.dynamic_slice_in_dim(source_factor, first, panels_local, 2).astype(jnp.float32)
        charges = lax.dynamic_slice_in_dim(field, first, panels_local, 1).astype(jnp.float32)
        return jnp.einsum('jrp,mp->jrm', factor, charges, precision=highest).astype(jnp.bfloat16)

    table = lax.map(coefficients, jnp.arange(row_total, dtype=jnp.int32))
    leaves = field.reshape(excite, leaf_total, leaf_size)

    def block_row(device):
        first_leaf = device * leaves_local
        tiles = lax.dynamic_slice_in_dim(near_tiles, first_leaf, leaves_local, 0).astype(jnp.float32)
        offsets = lax.dynamic_slice_in_dim(near_offset, first_leaf, leaves_local, 0)
        counts = lax.dynamic_slice_in_dim(near_count, first_leaf, leaves_local, 0)
        source_leaf = (first_leaf + jnp.arange(leaves_local, dtype=jnp.int32)[:, None] + offsets) % leaf_total
        picked = jnp.take(leaves, source_leaf.reshape(-1).astype(jnp.int32), axis=1)
        picked = picked.reshape(excite, leaves_local, near_slots, leaf_size).astype(jnp.float32)
        live_near = jnp.arange(near_slots, dtype=jnp.int32)[None, :] < counts[:, None]
        picked = jnp.where(live_near[None, :, :, None], picked, jnp.zeros_like(picked))
        near_part = jnp.einsum('ijab,mijb->mia', tiles, picked, precision=highest).reshape(excite, panels_local)
        sources = far_src[device]
        ranks = out_rank[device]
        live_slot = live_far[device]
        coef = table[sources, ranks].astype(jnp.float32)
        coef = jnp.where(live_slot[:, None, None], coef, jnp.zeros_like(coef))
        factor = lax.dynamic_slice_in_dim(target_factor, device * panels_local, panels_local, 2).astype(jnp.float32)
        far_part = jnp.einsum('jrm,jrp->mp', coef, factor, precision=highest)
        return near_part + far_part

    rows_out = lax.map(block_row, jnp.arange(row_total, dtype=jnp.int32))
    return jnp.transpose(rows_out, (1, 0, 2)).reshape(excite, row_total * panels_local)


def reference(excitation, near_tiles, near_offset, near_count, far_src, far_count, source_factor, target_factor):
    out_rank, live_far = out_ranks(far_src, far_count)
    current = excitation
    results = []
    for step in range(ITERS):
        result = apply_operator(current, near_tiles, near_offset, near_count, far_src, out_rank, live_far, source_factor, target_factor)
        results.append(result)
        current = result.astype(jnp.bfloat16)
    return jnp.stack(results, axis=0)
```

```python
import functools

import jax
import jax.numpy as jnp
from jax import lax
from jax.experimental import pallas as pl
from jax.experimental.pallas import tpu as pltpu
from jax.sharding import PartitionSpec as P

ITERS = 5
MESH = pl.DeviceIdType.MESH
NT = (((1,), (1,)), ((), ()))

SEND = (1, 0, 2, 3)
EARLY = 2
BUFFERS = ((0, 1), (2,), (3,))
STEPS = ((3, 2), (1,), (0,))
GROUPS = 4


def kernel(n, off_ref, cnt_ref, fsrc_ref, fcnt_ref, field_hbm, near_hbm, src_hbm, tgt_hbm, out, *scratch):
    (near, src, tgt, field, main_a, main_b, *rest) = scratch
    nbuf = len(BUFFERS)
    exts = (rest[:nbuf], rest[nbuf : 2 * nbuf])
    (
        recv_a,
        recv_b,
        outg_a,
        outg_b,
        cbuf,
        acc,
        near_tab,
        send_tab,
        recv_tab,
        load_sem,
        in_send,
        in_recv,
        ext_send,
        ext_recv,
        far_send,
        far_recv,
    ) = rest[2 * nbuf :]
    mains, recvs, outgs = (main_a, main_b), (recv_a, recv_b), (outg_a, outg_b)

    me = lax.axis_index("panels")
    core = lax.rem(me, 2)
    inner = me + 1 - 2 * core
    outer = lax.rem(me + n - 1 + 2 * core, n)
    leaves, slots = off_ref.shape
    excite, panels = field.shape
    leaf = panels // leaves
    size = leaves // GROUPS
    pack = cbuf.shape[1]
    far_slots = cbuf.shape[0] - 1
    half = far_slots * pack
    last = ITERS - 1

    barrier = pltpu.get_barrier_semaphore()

    @pl.loop(1, n)
    def _(d):
        pl.semaphore_signal(barrier, inc=1, device_id=(lax.rem(me + d, n),), device_id_type=MESH)

    load_field = pltpu.make_async_copy(field_hbm, field, load_sem.at[0])
    load_src = [
        pltpu.make_async_copy(src_hbm.at[:, pl.ds(h * pack, pack), :], src.at[h], load_sem.at[1 + h]) for h in range(2)
    ]
    load_tgt = [
        pltpu.make_async_copy(tgt_hbm.at[:, pl.ds(h * pack, pack), :], tgt.at[h], load_sem.at[3 + h]) for h in range(2)
    ]
    load_near = pltpu.make_async_copy(near_hbm, near, load_sem.at[5])
    for load in [load_field, *load_src, load_near, *load_tgt]:
        load.start()

    def base(group):
        return jnp.where(core == 1, leaves - (group + 1) * size, group * size)

    def columns(group):
        return pl.ds(pl.multiple_of(base(group) * leaf, size * leaf), size * leaf)

    def inner_copy(k, group):
        own = mains[k % 2]
        return pltpu.make_async_remote_copy(
            src_ref=own.at[pl.ds(base(group), size)],
            dst_ref=own.at[pl.ds(leaves + base(group), size)],
            send_sem=in_send.at[k % 2, group],
            recv_sem=in_recv.at[k % 2, group],
            device_id=(inner,),
            device_id_type=MESH,
        )

    def outer_copy(k, place):
        buffer = next(b for b, places in enumerate(BUFFERS) if place in places)
        return pltpu.make_async_remote_copy(
            src_ref=mains[k % 2].at[pl.ds(base(SEND[place]), size)],
            dst_ref=exts[k % 2][buffer].at[pl.ds(BUFFERS[buffer].index(place) * size, size)],
            send_sem=ext_send.at[k % 2, place],
            recv_sem=ext_recv.at[k % 2, place],
            device_id=(outer,),
            device_id_type=MESH,
        )

    def far_copy(k, d):
        peer = lax.rem(me + d, n)
        return pltpu.make_async_remote_copy(
            src_ref=outgs[k % 2].at[peer],
            dst_ref=recvs[k % 2].at[me],
            send_sem=far_send.at[k % 2, d],
            recv_sem=far_recv.at[k % 2, d],
            device_id=(peer,),
            device_id_type=MESH,
        )

    blank = jnp.zeros((excite, leaf), jnp.bfloat16)
    for buffers in (mains, *exts):
        for buffer in buffers:
            buffer[buffer.shape[0] - 1] = blank
    for recv in recvs:
        recv[n] = jnp.zeros((pack, 2 * excite), jnp.bfloat16)
        recv[me] = jnp.zeros((pack, 2 * excite), jnp.bfloat16)
    cbuf[far_slots] = jnp.zeros((pack, 2 * excite), jnp.bfloat16)

    load_field.wait()
    for i in range(leaves):
        main_a[i] = field[:, i * leaf : (i + 1) * leaf]
    pl.semaphore_wait(barrier, n - 1)
    for place in range(EARLY):
        outer_copy(0, place).start()
    for group in range(GROUPS):
        inner_copy(0, group).start()

    @pl.loop(0, leaves)
    def _(i):
        for j in range(slots):
            at = i + off_ref[i, j]
            live = j < cnt_ref[i]
            low, high = at < 0, at >= leaves
            far_side = jnp.where(core == 1, high.astype(jnp.int32), low.astype(jnp.int32)) == 1
            spot = jnp.where(low, at + leaves, jnp.where(high, at - leaves, at))
            own = jnp.logical_not(jnp.logical_or(low, high))
            near_side = jnp.where(own, spot, leaves + spot)
            use = jnp.logical_and(live, jnp.logical_not(far_side))
            near_tab[i * slots + j] = jnp.where(use, near_side, 2 * leaves)
            use = jnp.logical_and(live, far_side)
            for b, places in enumerate(BUFFERS):
                found = len(places) * size
                for order, place in enumerate(places):
                    group = SEND[place]
                    first = jnp.where(core == 1, group * size, leaves - (group + 1) * size)
                    inside = jnp.logical_and(spot >= first, spot < first + size)
                    inside = jnp.logical_and(inside, use)
                    found = jnp.where(inside, order * size + spot - first, found)
                near_tab[((b + 1) * leaves + i) * slots + j] = found

    def count(t, before):
        mine = 0
        live = fcnt_ref[t]
        for j in range(far_slots):
            mine += jnp.logical_and(fsrc_ref[t, j] == me, j < live).astype(jnp.int32)
        send_tab[t] = jnp.where(mine > 0, before, far_slots)
        return before + mine

    lax.fori_loop(0, n, count, jnp.int32(0))
    my_live = fcnt_ref[me]
    for j in range(far_slots):
        recv_tab[j] = jnp.where(j < my_live, fsrc_ref[me, j], n)

    def project(group, fresh):
        cols = columns(group)
        charges = field[:, cols]
        for h in range(2):
            part = lax.dot_general(
                src[h, :, :, cols].reshape(half, size * leaf), charges, NT, preferred_element_type=jnp.float32
            )
            acc[h] = part if fresh else acc[h] + part

    def send_far(k):
        both = jnp.concatenate([acc[0], acc[1]], axis=1)
        cbuf[:far_slots] = both.reshape(far_slots, pack, 2 * excite).astype(jnp.bfloat16)
        outg = outgs[k % 2]

        @pl.loop(0, n)
        def _(t):
            outg[t] = cbuf[send_tab[t]]

        @pl.loop(1, n)
        def _(d):
            far_copy(k, d).start()

        for place in range(EARLY, GROUPS):
            outer_copy(k, place).start()

    def near_sum(k, group, step):
        own, ext = mains[k % 2], exts[k % 2][: step + 1]
        sums = []
        for u in range(size):
            i = base(group) + u
            total = None
            for j in range(slots):
                x = own[near_tab[i * slots + j]]
                for b, buffer in enumerate(ext):
                    x += buffer[near_tab[((b + 1) * leaves + i) * slots + j]]
                part = lax.dot_general(x, near[i, j], NT, preferred_element_type=jnp.float32)
                total = part if total is None else total + part
            sums.append(total)
        return jnp.concatenate(sums, axis=1)

    def finish(k, group, total):
        cols = columns(group)
        out[k, :, cols] = total
        if k < last:
            rounded = total.astype(jnp.bfloat16)
            field[:, cols] = rounded
            for u in range(size):
                mains[(k + 1) % 2][base(group) + u] = rounded[:, u * leaf : (u + 1) * leaf]

    for load in load_src:
        load.wait()
    for group in range(GROUPS):
        project(group, group == 0)
    send_far(0)

    for k in range(ITERS):
        for group in range(GROUPS):
            inner_copy(k, group).wait_recv()
        for place in BUFFERS[0]:
            outer_copy(k, place).wait_recv()
        if k == 0:
            load_near.wait()
        for group in STEPS[0]:
            out[k, :, columns(group)] = near_sum(k, group, 0)

        @pl.loop(1, n)
        def _(d):
            far_copy(k, d).wait()

        got = jnp.concatenate([recvs[k % 2][recv_tab[j]] for j in range(far_slots)], axis=0)
        got = got.astype(jnp.float32).T.astype(jnp.bfloat16)
        coef = jnp.concatenate([got[:excite], got[excite:]], axis=1)
        if k == 0:
            for load in load_tgt:
                load.wait()
        if 1 <= k < last:
            for place in range(GROUPS):
                outer_copy(k - 1, place).wait_send()
            for group in range(GROUPS):
                inner_copy(k - 1, group).wait_send()

        def far_sum(group):
            cols = columns(group)
            return jnp.dot(coef, tgt[:, :, :, cols].reshape(2 * half, size * leaf), preferred_element_type=jnp.float32)

        for group in STEPS[0]:
            finish(k, group, out[k, :, columns(group)] + far_sum(group))
            if k < last:
                inner_copy(k + 1, group).start()
        for step in STEPS[1:]:
            for group in step:
                out[k, :, columns(group)] = far_sum(group)
        if k < last:
            for at, group in enumerate(STEPS[0]):
                project(group, at == 0)
        for step in range(1, nbuf):
            for place in BUFFERS[step]:
                outer_copy(k, place).wait_recv()
            for group in STEPS[step]:
                finish(k, group, near_sum(k, group, step) + out[k, :, columns(group)])
                if k < last:
                    if group in SEND[:EARLY]:
                        outer_copy(k + 1, SEND.index(group)).start()
                    inner_copy(k + 1, group).start()
                    project(group, False)
        if k < last:
            send_far(k + 1)
    for k in range(max(ITERS - 2, 0), ITERS):
        for place in range(GROUPS):
            outer_copy(k, place).wait_send()
        for group in range(GROUPS):
            inner_copy(k, group).wait_send()


def shards(n, excitation, near_tiles, near_offset, near_count, far_src, far_count, source_factor, target_factor):
    excite, panels = excitation.shape
    leaves, slots, leaf, _ = near_tiles.shape
    far_slots, rank, _ = source_factor.shape
    size, pack = leaves // GROUPS, rank // 2
    bf, f32 = jnp.bfloat16, jnp.float32
    hbm = pl.BlockSpec(memory_space=pltpu.HBM)
    smem = pl.BlockSpec(memory_space=pltpu.SMEM)
    ext = [pltpu.VMEM((len(places) * size + 1, excite, leaf), bf) for places in BUFFERS]
    return pl.pallas_call(
        functools.partial(kernel, n),
        out_shape=pltpu.VMEM((ITERS, excite, panels), f32),
        in_specs=[smem] * 4 + [hbm] * 4,
        out_specs=pl.BlockSpec(memory_space=pltpu.VMEM),
        scratch_shapes=[
            pltpu.VMEM((leaves, slots, leaf, leaf), bf),
            pltpu.VMEM((2, far_slots, pack, panels), bf),
            pltpu.VMEM((2, far_slots, pack, panels), bf),
            pltpu.VMEM((excite, panels), bf),
            pltpu.VMEM((2 * leaves + 1, excite, leaf), bf),
            pltpu.VMEM((2 * leaves + 1, excite, leaf), bf),
            *ext,
            *ext,
            pltpu.VMEM((n + 1, pack, 2 * excite), bf),
            pltpu.VMEM((n + 1, pack, 2 * excite), bf),
            pltpu.VMEM((n, pack, 2 * excite), bf),
            pltpu.VMEM((n, pack, 2 * excite), bf),
            pltpu.VMEM((far_slots + 1, pack, 2 * excite), bf),
            pltpu.VMEM((2, far_slots * pack, excite), f32),
            pltpu.SMEM(((1 + len(BUFFERS)) * leaves * slots,), jnp.int32),
            pltpu.SMEM((n,), jnp.int32),
            pltpu.SMEM((far_slots,), jnp.int32),
            pltpu.SemaphoreType.DMA((6,)),
            pltpu.SemaphoreType.DMA((2, GROUPS)),
            pltpu.SemaphoreType.DMA((2, GROUPS)),
            pltpu.SemaphoreType.DMA((2, GROUPS)),
            pltpu.SemaphoreType.DMA((2, GROUPS)),
            pltpu.SemaphoreType.DMA((2, n)),
            pltpu.SemaphoreType.DMA((2, n)),
        ],
        compiler_params=pltpu.CompilerParams(
            collective_id=0, has_side_effects=True, vmem_limit_bytes=54 * 1024 * 1024
        ),
    )(near_offset, near_count, far_src, far_count, excitation, near_tiles, source_factor, target_factor)


def solution(mesh):
    in_specs = (
        P(None, "panels"),
        P("panels", None, None, None),
        P("panels", None),
        P("panels"),
        P(),
        P(),
        P(None, None, "panels"),
        P(None, None, "panels"),
    )
    return jax.shard_map(
        functools.partial(shards, mesh.shape["panels"]),
        mesh=mesh,
        in_specs=in_specs,
        out_specs=P(None, None, "panels"),
        check_vma=False,
    )
```

```python
import functools

import jax
import jax.numpy as jnp
from jax import lax
from jax.experimental import pallas as pl
from jax.experimental.pallas import tpu as pltpu
from jax.sharding import PartitionSpec as P

ITERS = 5
MESH = pl.DeviceIdType.MESH
NT = (((1,), (1,)), ((), ()))

SEND = (1, 0, 2, 3)
BUFFERS = ((0, 1), (2,), (3,))
NEED = (2, 1, 0, 0)
GROUPS = 4


def kernel(n, off_hbm, cnt_hbm, fsrc_hbm, fcnt_hbm, field_hbm, near_hbm, src_hbm, tgt_hbm, out, *scratch):
    off_ref, cnt_ref, fsrc_ref, fcnt_ref, near, src, tgt, field, main_a, main_b, *rest = scratch
    nbuf = len(BUFFERS)
    exts = (rest[:nbuf], rest[nbuf : 2 * nbuf])
    (
        recv_a,
        recv_b,
        outg_a,
        outg_b,
        cbuf,
        acc,
        near_tab,
        send_tab,
        recv_tab,
        load_sem,
        in_send,
        in_recv,
        ext_send,
        ext_recv,
        far_send,
        far_recv,
    ) = rest[2 * nbuf :]
    mains, recvs, outgs = (main_a, main_b), (recv_a, recv_b), (outg_a, outg_b)

    me = lax.axis_index("panels")
    core = lax.rem(me, 2)
    inner = me + 1 - 2 * core
    outer = lax.rem(me + n - 1 + 2 * core, n)
    slots, leaves = off_ref.shape
    excite, panels = field.shape
    leaf = panels // leaves
    size = leaves // GROUPS
    pack = cbuf.shape[1]
    far_slots = cbuf.shape[0] - 1
    half = far_slots * pack
    last = ITERS - 1

    barrier = pltpu.get_barrier_semaphore()

    @pl.loop(1, n)
    def _(d):
        pl.semaphore_signal(barrier, inc=1, device_id=(lax.rem(me + d, n),), device_id_type=MESH)

    load_field = pltpu.make_async_copy(field_hbm, field, load_sem.at[0])
    load_src = [
        pltpu.make_async_copy(src_hbm.at[:, pl.ds(h * pack, pack), :], src.at[h], load_sem.at[1 + h]) for h in range(2)
    ]
    load_tgt = [
        pltpu.make_async_copy(tgt_hbm.at[:, pl.ds(h * pack, pack), :], tgt.at[h], load_sem.at[3 + h]) for h in range(2)
    ]
    load_near = pltpu.make_async_copy(near_hbm, near, load_sem.at[5])
    load_ints = [
        pltpu.make_async_copy(a, b, load_sem.at[6 + i])
        for i, (a, b) in enumerate(
            ((off_hbm, off_ref), (cnt_hbm, cnt_ref), (fsrc_hbm, fsrc_ref), (fcnt_hbm, fcnt_ref))
        )
    ]
    for load in [load_field, *load_ints, *load_src, load_near, *load_tgt]:
        load.start()

    def base(group):
        return jnp.where(core == 1, leaves - (group + 1) * size, group * size)

    def columns(group):
        return pl.ds(pl.multiple_of(base(group) * leaf, size * leaf), size * leaf)

    def inner_copy(k, group):
        own = mains[k % 2]
        return pltpu.make_async_remote_copy(
            src_ref=own.at[pl.ds(base(group), size)],
            dst_ref=own.at[pl.ds(leaves + base(group), size)],
            send_sem=in_send.at[k % 2, group],
            recv_sem=in_recv.at[k % 2, group],
            device_id=(inner,),
            device_id_type=MESH,
        )

    def outer_copy(k, place):
        buffer = next(b for b, places in enumerate(BUFFERS) if place in places)
        return pltpu.make_async_remote_copy(
            src_ref=mains[k % 2].at[pl.ds(base(SEND[place]), size)],
            dst_ref=exts[k % 2][buffer].at[pl.ds(BUFFERS[buffer].index(place) * size, size)],
            send_sem=ext_send.at[k % 2, place],
            recv_sem=ext_recv.at[k % 2, place],
            device_id=(outer,),
            device_id_type=MESH,
        )

    def far_copy(k, d):
        peer = lax.rem(me + d, n)
        return pltpu.make_async_remote_copy(
            src_ref=outgs[k % 2].at[peer],
            dst_ref=recvs[k % 2].at[me],
            send_sem=far_send.at[k % 2, d],
            recv_sem=far_recv.at[k % 2, d],
            device_id=(peer,),
            device_id_type=MESH,
        )

    blank = jnp.zeros((excite, leaf), jnp.bfloat16)
    for buffers in (mains, *exts):
        for buffer in buffers:
            buffer[buffer.shape[0] - 1] = blank
    for recv in recvs:
        recv[n] = jnp.zeros((pack, 2 * excite), jnp.bfloat16)
        recv[me] = jnp.zeros((pack, 2 * excite), jnp.bfloat16)
    cbuf[far_slots] = jnp.zeros((pack, 2 * excite), jnp.bfloat16)

    for load in load_ints:
        load.wait()

    def count(t, before):
        mine = 0
        live = fcnt_ref[t]
        for j in range(far_slots):
            mine += jnp.logical_and(fsrc_ref[j, t] == me, j < live).astype(jnp.int32)
        send_tab[t] = jnp.where(mine > 0, before, far_slots)
        return before + mine

    lax.fori_loop(0, n, count, jnp.int32(0))
    my_live = fcnt_ref[me]
    for j in range(far_slots):
        recv_tab[j] = jnp.where(j < my_live, fsrc_ref[j, me], n)

    load_field.wait()
    for i in range(leaves):
        main_a[i] = field[:, i * leaf : (i + 1) * leaf]
    pl.semaphore_wait(barrier, n - 1)
    for place in (0, 1):
        outer_copy(0, place).start()
    for group in range(GROUPS):
        inner_copy(0, group).start()

    def near_table():
        @pl.loop(0, leaves)
        def _(i):
            for j in range(slots):
                at = i + off_ref[j, i]
                live = j < cnt_ref[i]
                low, high = at < 0, at >= leaves
                far_side = jnp.where(core == 1, high.astype(jnp.int32), low.astype(jnp.int32)) == 1
                spot = jnp.where(low, at + leaves, jnp.where(high, at - leaves, at))
                own = jnp.logical_not(jnp.logical_or(low, high))
                near_side = jnp.where(own, spot, leaves + spot)
                use = jnp.logical_and(live, jnp.logical_not(far_side))
                near_tab[i * slots + j] = jnp.where(use, near_side, 2 * leaves)
                use = jnp.logical_and(live, far_side)
                for b, places in enumerate(BUFFERS):
                    found = len(places) * size
                    for order, place in enumerate(places):
                        group = SEND[place]
                        first = jnp.where(core == 1, group * size, leaves - (group + 1) * size)
                        inside = jnp.logical_and(spot >= first, spot < first + size)
                        inside = jnp.logical_and(inside, use)
                        found = jnp.where(inside, order * size + spot - first, found)
                    near_tab[((b + 1) * leaves + i) * slots + j] = found

    def project(group, fresh):
        cols = columns(group)
        charges = field[:, cols]
        for h in range(2):
            part = lax.dot_general(
                src[h, :, :, cols].reshape(half, size * leaf), charges, NT, preferred_element_type=jnp.float32
            )
            acc[h] = part if fresh else acc[h] + part

    def send_far(k):
        both = jnp.concatenate([acc[0], acc[1]], axis=1)
        cbuf[:far_slots] = both.reshape(far_slots, pack, 2 * excite).astype(jnp.bfloat16)
        outg = outgs[k % 2]

        @pl.loop(0, n)
        def _(t):
            outg[t] = cbuf[send_tab[t]]

        @pl.loop(1, n)
        def _(d):
            far_copy(k, d).start()

    def near_sum(k, group):
        own, ext = mains[k % 2], exts[k % 2][: NEED[group] + 1]
        sums = []
        for u in range(size):
            i = base(group) + u
            total = None
            for j in range(slots):
                x = own[near_tab[i * slots + j]]
                for b, buffer in enumerate(ext):
                    x += buffer[near_tab[((b + 1) * leaves + i) * slots + j]]
                part = jnp.dot(x, near[i, j], preferred_element_type=jnp.float32)
                total = part if total is None else total + part
            sums.append(total)
        return jnp.concatenate(sums, axis=1)

    def far_sum(coef, group):
        rows = tgt[:, :, :, columns(group)].reshape(2 * half, size * leaf)
        return jnp.dot(coef, rows, preferred_element_type=jnp.float32)

    def finish(k, group, total):
        cols = columns(group)
        out[k, :, cols] = total
        if k < last:
            rounded = total.astype(jnp.bfloat16)
            field[:, cols] = rounded
            for u in range(size):
                mains[(k + 1) % 2][base(group) + u] = rounded[:, u * leaf : (u + 1) * leaf]
            inner_copy(k + 1, group).start()
            if group in SEND[:2]:
                outer_copy(k + 1, SEND.index(group)).start()

    def wait_sent(k):
        for place in range(GROUPS):
            outer_copy(k, place).wait_send()
        for group in range(GROUPS):
            inner_copy(k, group).wait_send()

    for load in load_src:
        load.wait()
    for group in range(GROUPS):
        project(group, group == 0)

    for k in range(ITERS):
        part = {}

        def add_near(group):
            part[group] = True
            cols = columns(group)
            total = near_sum(k, group)
            if group in far_done:
                finish(k, group, total + out[k, :, cols])
            else:
                out[k, :, cols] = total

        def add_far(coef, group):
            far_done.add(group)
            cols = columns(group)
            total = far_sum(coef, group)
            if group in part:
                finish(k, group, total + out[k, :, cols])
            else:
                out[k, :, cols] = total

        far_done = set()
        send_far(k)
        outer_copy(k, 2).start()
        outer_copy(k, 3).start()
        if k == 0:
            near_table()
            load_near.wait()

            @pl.loop(0, leaves)
            def _(i):
                for j in range(slots):
                    near[i, j] = near[i, j].T

        for group in range(GROUPS):
            inner_copy(k, group).wait_recv()
        for place in (0, 1):
            outer_copy(k, place).wait_recv()
        add_near(3)
        if k < last:
            outer_copy(k, 2).wait_recv()
            add_near(1)
        else:
            add_near(2)

        @pl.loop(1, n)
        def _(d):
            far_copy(k, d).wait()

        got = jnp.concatenate([recvs[k % 2][recv_tab[j]] for j in range(far_slots)], axis=0)
        got = got.astype(jnp.float32).T.astype(jnp.bfloat16)
        coef = jnp.concatenate([got[:excite], got[excite:]], axis=1)
        if k == 0:
            for load in load_tgt:
                load.wait()
        if 1 <= k < last:
            wait_sent(k - 1)
        if k < last:
            add_far(coef, 1)
            add_far(coef, 0)
            add_near(2)
            outer_copy(k, 3).wait_recv()
            add_near(0)
            add_far(coef, 3)
            add_far(coef, 2)
            for at, group in enumerate((1, 3, 2, 0)):
                project(group, at == 0)
        else:
            for group in (3, 2, 1, 0):
                add_far(coef, group)
            outer_copy(k, 2).wait_recv()
            add_near(1)
            outer_copy(k, 3).wait_recv()
            add_near(0)
    for k in range(max(ITERS - 2, 0), ITERS):
        wait_sent(k)


def shards(n, excitation, near_tiles, near_offset, near_count, far_src, far_count, source_factor, target_factor):
    excite, panels = excitation.shape
    leaves, slots, leaf, _ = near_tiles.shape
    far_slots, rank, _ = source_factor.shape
    size, pack = leaves // GROUPS, rank // 2
    bf, f32 = jnp.bfloat16, jnp.float32
    hbm = pl.BlockSpec(memory_space=pltpu.HBM)
    ext = [pltpu.VMEM((len(places) * size + 1, excite, leaf), bf) for places in BUFFERS]
    return pl.pallas_call(
        functools.partial(kernel, n),
        out_shape=pltpu.VMEM((ITERS, excite, panels), f32),
        in_specs=[hbm] * 8,
        out_specs=pl.BlockSpec(memory_space=pltpu.VMEM),
        scratch_shapes=[
            pltpu.SMEM((slots, leaves), jnp.int32),
            pltpu.SMEM((leaves,), jnp.int32),
            pltpu.SMEM((far_slots, n), jnp.int32),
            pltpu.SMEM((n,), jnp.int32),
            pltpu.VMEM((leaves, slots, leaf, leaf), bf),
            pltpu.VMEM((2, far_slots, pack, panels), bf),
            pltpu.VMEM((2, far_slots, pack, panels), bf),
            pltpu.VMEM((excite, panels), bf),
            pltpu.VMEM((2 * leaves + 1, excite, leaf), bf),
            pltpu.VMEM((2 * leaves + 1, excite, leaf), bf),
            *ext,
            *ext,
            pltpu.VMEM((n + 1, pack, 2 * excite), bf),
            pltpu.VMEM((n + 1, pack, 2 * excite), bf),
            pltpu.VMEM((n, pack, 2 * excite), bf),
            pltpu.VMEM((n, pack, 2 * excite), bf),
            pltpu.VMEM((far_slots + 1, pack, 2 * excite), bf),
            pltpu.VMEM((2, far_slots * pack, excite), f32),
            pltpu.SMEM(((1 + len(BUFFERS)) * leaves * slots,), jnp.int32),
            pltpu.SMEM((n,), jnp.int32),
            pltpu.SMEM((far_slots,), jnp.int32),
            pltpu.SemaphoreType.DMA((10,)),
            pltpu.SemaphoreType.DMA((2, GROUPS)),
            pltpu.SemaphoreType.DMA((2, GROUPS)),
            pltpu.SemaphoreType.DMA((2, GROUPS)),
            pltpu.SemaphoreType.DMA((2, GROUPS)),
            pltpu.SemaphoreType.DMA((2, n)),
            pltpu.SemaphoreType.DMA((2, n)),
        ],
        compiler_params=pltpu.CompilerParams(
            collective_id=0, has_side_effects=True, vmem_limit_bytes=54 * 1024 * 1024
        ),
    )(near_offset.T, near_count, far_src.T, far_count, excitation, near_tiles, source_factor, target_factor)


def solution(mesh):
    in_specs = (
        P(None, "panels"),
        P("panels", None, None, None),
        P("panels", None),
        P("panels"),
        P(),
        P(),
        P(None, None, "panels"),
        P(None, None, "panels"),
    )
    return jax.shard_map(
        functools.partial(shards, mesh.shape["panels"]),
        mesh=mesh,
        in_specs=in_specs,
        out_specs=P(None, None, "panels"),
        check_vma=False,
    )
```

```python
import functools

import jax
import jax.numpy as jnp
from jax import lax
from jax.experimental import pallas as pl
from jax.experimental.pallas import tpu as pltpu
from jax.sharding import PartitionSpec as P

ITERS = 5
MESH = pl.DeviceIdType.MESH
NT = (((1,), (1,)), ((), ()))

SEND = (1, 0, 2, 3)
BUFFERS = ((0, 1), (2,), (3,))
NEED = (2, 1, 0, 0)
GROUPS = 4


def kernel(n, off_hbm, cnt_hbm, fsrc_hbm, fcnt_hbm, field_hbm, near_hbm, src_hbm, tgt_hbm, out, *scratch):
    off_ref, cnt_ref, fsrc_ref, fcnt_ref, near, src, tgt, field, main_a, main_b, *rest = scratch
    nbuf = len(BUFFERS)
    exts = (rest[:nbuf], rest[nbuf : 2 * nbuf])
    (
        recv_a,
        recv_b,
        outg_a,
        outg_b,
        cbuf,
        acc,
        near_tab,
        send_tab,
        recv_tab,
        load_sem,
        in_send,
        in_recv,
        ext_send,
        ext_recv,
        far_send,
        far_recv,
    ) = rest[2 * nbuf :]
    mains, recvs, outgs = (main_a, main_b), (recv_a, recv_b), (outg_a, outg_b)

    me = lax.axis_index("panels")
    core = lax.rem(me, 2)
    inner = me + 1 - 2 * core
    outer = lax.rem(me + n - 1 + 2 * core, n)
    slots, leaves = off_ref.shape
    excite, panels = field.shape
    leaf = panels // leaves
    size = leaves // GROUPS
    pack = cbuf.shape[1]
    far_slots = cbuf.shape[0] - 1
    half = far_slots * pack
    last = ITERS - 1

    barrier = pltpu.get_barrier_semaphore()

    load_field = pltpu.make_async_copy(field_hbm, field, load_sem.at[0])
    load_field.start()

    @pl.loop(1, n)
    def _(d):
        pl.semaphore_signal(barrier, inc=1, device_id=(lax.rem(me + d, n),), device_id_type=MESH)

    load_src = [
        pltpu.make_async_copy(src_hbm.at[:, pl.ds(h * pack, pack), :], src.at[h], load_sem.at[1 + h]) for h in range(2)
    ]
    load_tgt = [
        pltpu.make_async_copy(tgt_hbm.at[:, pl.ds(h * pack, pack), :], tgt.at[h], load_sem.at[3 + h]) for h in range(2)
    ]
    load_near = pltpu.make_async_copy(near_hbm, near, load_sem.at[5])
    load_ints = [
        pltpu.make_async_copy(a, b, load_sem.at[6 + i])
        for i, (a, b) in enumerate(
            ((off_hbm, off_ref), (cnt_hbm, cnt_ref), (fsrc_hbm, fsrc_ref), (fcnt_hbm, fcnt_ref))
        )
    ]
    for load in [*load_ints, *load_src]:
        load.start()

    def base(group):
        return jnp.where(core == 1, leaves - (group + 1) * size, group * size)

    def columns(group):
        return pl.ds(pl.multiple_of(base(group) * leaf, size * leaf), size * leaf)

    def taken(ref, sem):
        pltpu.make_async_copy(ref, ref, sem).wait()

    def inner_copy(k, group):
        own = mains[k % 2]
        return pltpu.make_async_remote_copy(
            src_ref=own.at[pl.ds(base(group), size)],
            dst_ref=own.at[pl.ds(leaves + base(group), size)],
            send_sem=in_send.at[k % 2],
            recv_sem=in_recv.at[k % 2],
            device_id=(inner,),
            device_id_type=MESH,
        )

    def outer_copy(k, place):
        buffer = next(b for b, places in enumerate(BUFFERS) if place in places)
        return pltpu.make_async_remote_copy(
            src_ref=mains[k % 2].at[pl.ds(base(SEND[place]), size)],
            dst_ref=exts[k % 2][buffer].at[pl.ds(BUFFERS[buffer].index(place) * size, size)],
            send_sem=ext_send.at[k % 2],
            recv_sem=ext_recv.at[k % 2, place],
            device_id=(outer,),
            device_id_type=MESH,
        )

    def far_copy(k, d):
        peer = lax.rem(me + d, n)
        return pltpu.make_async_remote_copy(
            src_ref=outgs[k % 2].at[peer],
            dst_ref=recvs[k % 2].at[me],
            send_sem=far_send.at[k % 2],
            recv_sem=far_recv.at[k % 2],
            device_id=(peer,),
            device_id_type=MESH,
        )

    blank = jnp.zeros((excite, leaf), jnp.bfloat16)
    for buffers in (mains, *exts):
        for buffer in buffers:
            buffer[buffer.shape[0] - 1] = blank
    for recv in recvs:
        recv[n] = jnp.zeros((pack, 2 * excite), jnp.bfloat16)
        recv[me] = jnp.zeros((pack, 2 * excite), jnp.bfloat16)
    cbuf[far_slots] = jnp.zeros((pack, 2 * excite), jnp.bfloat16)

    load_field.wait()
    for i in range(leaves):
        main_a[i] = field[:, i * leaf : (i + 1) * leaf]
    for load in [load_near, *load_tgt]:
        load.start()
    pl.semaphore_wait(barrier, n - 1)
    for place in (0, 1):
        outer_copy(0, place).start()
    for group in range(GROUPS):
        inner_copy(0, group).start()

    for load in load_ints:
        load.wait()

    def count(t, before):
        mine = 0
        live = fcnt_ref[t]
        for j in range(far_slots):
            mine += jnp.logical_and(fsrc_ref[j, t] == me, j < live).astype(jnp.int32)
        send_tab[t] = jnp.where(mine > 0, before, far_slots)
        return before + mine

    lax.fori_loop(0, n, count, jnp.int32(0))
    my_live = fcnt_ref[me]
    for j in range(far_slots):
        recv_tab[j] = jnp.where(j < my_live, fsrc_ref[j, me], n)

    def near_table():
        @pl.loop(0, leaves)
        def _(i):
            for j in range(slots):
                at = i + off_ref[j, i]
                live = j < cnt_ref[i]
                low, high = at < 0, at >= leaves
                far_side = jnp.where(core == 1, high.astype(jnp.int32), low.astype(jnp.int32)) == 1
                spot = jnp.where(low, at + leaves, jnp.where(high, at - leaves, at))
                own = jnp.logical_not(jnp.logical_or(low, high))
                near_side = jnp.where(own, spot, leaves + spot)
                use = jnp.logical_and(live, jnp.logical_not(far_side))
                near_tab[i * slots + j] = jnp.where(use, near_side, 2 * leaves)
                use = jnp.logical_and(live, far_side)
                for b, places in enumerate(BUFFERS):
                    found = len(places) * size
                    for order, place in enumerate(places):
                        group = SEND[place]
                        first = jnp.where(core == 1, group * size, leaves - (group + 1) * size)
                        inside = jnp.logical_and(spot >= first, spot < first + size)
                        inside = jnp.logical_and(inside, use)
                        found = jnp.where(inside, order * size + spot - first, found)
                    near_tab[((b + 1) * leaves + i) * slots + j] = found

    def project(group, fresh):
        cols = columns(group)
        charges = field[:, cols]
        for h in range(2):
            part = lax.dot_general(
                src[h, :, :, cols].reshape(half, size * leaf), charges, NT, preferred_element_type=jnp.float32
            )
            acc[h] = part if fresh else acc[h] + part

    def send_far(k):
        both = jnp.concatenate([acc[0], acc[1]], axis=1)
        cbuf[:far_slots] = both.reshape(far_slots, pack, 2 * excite).astype(jnp.bfloat16)
        outg = outgs[k % 2]

        @pl.loop(0, n)
        def _(t):
            outg[t] = cbuf[send_tab[t]]

        @pl.loop(1, n)
        def _(d):
            far_copy(k, n - d).start()

    def near_sum(k, group):
        own, ext = mains[k % 2], exts[k % 2][: NEED[group] + 1]
        sums = []
        for u in range(size):
            i = base(group) + u
            total = None
            for j in range(slots):
                x = own[near_tab[i * slots + j]]
                for b, buffer in enumerate(ext):
                    x += buffer[near_tab[((b + 1) * leaves + i) * slots + j]]
                part = jnp.dot(x, near[i, j], preferred_element_type=jnp.float32)
                total = part if total is None else total + part
            sums.append(total)
        return jnp.concatenate(sums, axis=1)

    def far_sum(coef, group):
        rows = tgt[:, :, :, columns(group)].reshape(2 * half, size * leaf)
        return jnp.dot(coef, rows, preferred_element_type=jnp.float32)

    def finish(k, group, total):
        cols = columns(group)
        out[k, :, cols] = total
        if k < last:
            rounded = total.astype(jnp.bfloat16)
            field[:, cols] = rounded
            for u in range(size):
                mains[(k + 1) % 2][base(group) + u] = rounded[:, u * leaf : (u + 1) * leaf]
            inner_copy(k + 1, group).start()
            if group in SEND[:2]:
                outer_copy(k + 1, SEND.index(group)).start()

    def wait_sent(k):
        own = mains[k % 2].at[pl.ds(0, leaves)]
        taken(own, ext_send.at[k % 2])
        taken(own, in_send.at[k % 2])

    for load in load_src:
        load.wait()
    for group in range(GROUPS):
        project(group, group == 0)

    for k in range(ITERS):
        part = {}

        def add_near(group):
            part[group] = True
            cols = columns(group)
            total = near_sum(k, group)
            if group in far_done:
                finish(k, group, total + out[k, :, cols])
            else:
                out[k, :, cols] = total

        def add_far(coef, group):
            far_done.add(group)
            cols = columns(group)
            total = far_sum(coef, group)
            if group in part:
                finish(k, group, total + out[k, :, cols])
            else:
                out[k, :, cols] = total

        far_done = set()
        send_far(k)
        outer_copy(k, 2).start()
        outer_copy(k, 3).start()
        if k == 0:
            near_table()
            load_near.wait()

            @pl.loop(0, leaves)
            def _(i):
                for j in range(slots):
                    near[i, j] = near[i, j].T

        taken(mains[k % 2].at[pl.ds(0, leaves)], in_recv.at[k % 2])
        for place in (0, 1):
            outer_copy(k, place).wait_recv()
        add_near(3)
        add_near(2)
        outer_copy(k, 2).wait_recv()
        add_near(1)

        whole = recvs[k % 2].at[pl.ds(0, n - 1)]
        taken(whole, far_send.at[k % 2])
        taken(whole, far_recv.at[k % 2])

        got = jnp.concatenate([recvs[k % 2][recv_tab[j]] for j in range(far_slots)], axis=0)
        got = got.astype(jnp.float32).T.astype(jnp.bfloat16)
        coef = jnp.concatenate([got[:excite], got[excite:]], axis=1)
        if k == 0:
            for load in load_tgt:
                load.wait()
        if 1 <= k < last:
            wait_sent(k - 1)
        if k < last:
            add_far(coef, 1)
            add_far(coef, 0)
            outer_copy(k, 3).wait_recv()
            add_near(0)
            add_far(coef, 3)
            add_far(coef, 2)
            for at, group in enumerate((1, 3, 2, 0)):
                project(group, at == 0)
        else:
            for group in (3, 2, 1, 0):
                add_far(coef, group)
            outer_copy(k, 3).wait_recv()
            add_near(0)
    for k in range(max(ITERS - 2, 0), ITERS):
        wait_sent(k)


def shards(n, excitation, near_tiles, near_offset, near_count, far_src, far_count, source_factor, target_factor):
    excite, panels = excitation.shape
    leaves, slots, leaf, _ = near_tiles.shape
    far_slots, rank, _ = source_factor.shape
    size, pack = leaves // GROUPS, rank // 2
    bf, f32 = jnp.bfloat16, jnp.float32
    hbm = pl.BlockSpec(memory_space=pltpu.HBM)
    ext = [pltpu.VMEM((len(places) * size + 1, excite, leaf), bf) for places in BUFFERS]
    return pl.pallas_call(
        functools.partial(kernel, n),
        out_shape=pltpu.VMEM((ITERS, excite, panels), f32),
        in_specs=[hbm] * 8,
        out_specs=pl.BlockSpec(memory_space=pltpu.VMEM),
        scratch_shapes=[
            pltpu.SMEM((slots, leaves), jnp.int32),
            pltpu.SMEM((leaves,), jnp.int32),
            pltpu.SMEM((far_slots, n), jnp.int32),
            pltpu.SMEM((n,), jnp.int32),
            pltpu.VMEM((leaves, slots, leaf, leaf), bf),
            pltpu.VMEM((2, far_slots, pack, panels), bf),
            pltpu.VMEM((2, far_slots, pack, panels), bf),
            pltpu.VMEM((excite, panels), bf),
            pltpu.VMEM((2 * leaves + 1, excite, leaf), bf),
            pltpu.VMEM((2 * leaves + 1, excite, leaf), bf),
            *ext,
            *ext,
            pltpu.VMEM((n + 1, pack, 2 * excite), bf),
            pltpu.VMEM((n + 1, pack, 2 * excite), bf),
            pltpu.VMEM((n, pack, 2 * excite), bf),
            pltpu.VMEM((n, pack, 2 * excite), bf),
            pltpu.VMEM((far_slots + 1, pack, 2 * excite), bf),
            pltpu.VMEM((2, far_slots * pack, excite), f32),
            pltpu.SMEM(((1 + len(BUFFERS)) * leaves * slots,), jnp.int32),
            pltpu.SMEM((n,), jnp.int32),
            pltpu.SMEM((far_slots,), jnp.int32),
            pltpu.SemaphoreType.DMA((10,)),
            pltpu.SemaphoreType.DMA((2,)),
            pltpu.SemaphoreType.DMA((2,)),
            pltpu.SemaphoreType.DMA((2,)),
            pltpu.SemaphoreType.DMA((2, GROUPS)),
            pltpu.SemaphoreType.DMA((2,)),
            pltpu.SemaphoreType.DMA((2,)),
        ],
        compiler_params=pltpu.CompilerParams(
            collective_id=0, has_side_effects=True, vmem_limit_bytes=54 * 1024 * 1024
        ),
    )(near_offset.T, near_count, far_src.T, far_count, excitation, near_tiles, source_factor, target_factor)


def solution(mesh):
    in_specs = (
        P(None, "panels"),
        P("panels", None, None, None),
        P("panels", None),
        P("panels"),
        P(),
        P(),
        P(None, None, "panels"),
        P(None, None, "panels"),
    )
    return jax.shard_map(
        functools.partial(shards, mesh.shape["panels"]),
        mesh=mesh,
        in_specs=in_specs,
        out_specs=P(None, None, "panels"),
        check_vma=False,
    )
```

```python
import functools

import jax
import jax.numpy as jnp
from jax import lax
from jax.experimental import pallas as pl
from jax.experimental.pallas import tpu as pltpu
from jax.sharding import PartitionSpec as P

ITERS = 5
MESH = pl.DeviceIdType.MESH
NT = (((1,), (1,)), ((), ()))

SEND = (1, 0, 2, 3)
BUFFERS = ((0, 1), (2,), (3,))
NEED = (2, 1, 0, 0)
GROUPS = 4


def kernel(n, off_hbm, cnt_hbm, fsrc_hbm, fcnt_hbm, field_hbm, near_hbm, src_hbm, tgt_hbm, out, *scratch):
    off_ref, cnt_ref, fsrc_ref, fcnt_ref, near, src, tgt, field, main_a, main_b, *rest = scratch
    nbuf = len(BUFFERS)
    exts = (rest[:nbuf], rest[nbuf : 2 * nbuf])
    (
        recv_a,
        recv_b,
        outg_a,
        outg_b,
        cbuf,
        acc,
        near_tab,
        send_tab,
        recv_tab,
        load_sem,
        in_send,
        in_recv,
        ext_send,
        ext_recv,
        far_send,
        far_recv,
    ) = rest[2 * nbuf :]
    mains, recvs, outgs = (main_a, main_b), (recv_a, recv_b), (outg_a, outg_b)

    me = lax.axis_index("panels")
    core = lax.rem(me, 2)
    inner = me + 1 - 2 * core
    outer = lax.rem(me + n - 1 + 2 * core, n)
    slots, leaves = off_ref.shape
    excite, panels = field.shape
    leaf = panels // leaves
    size = leaves // GROUPS
    pack = cbuf.shape[1]
    far_slots = cbuf.shape[0] - 1
    half = far_slots * pack
    last = ITERS - 1

    barrier = pltpu.get_barrier_semaphore()

    load_field = pltpu.make_async_copy(field_hbm, field, load_sem.at[0])
    load_field.start()

    @pl.loop(1, n)
    def _(d):
        pl.semaphore_signal(barrier, inc=1, device_id=(lax.rem(me + d, n),), device_id_type=MESH)

    load_src = [
        pltpu.make_async_copy(src_hbm.at[:, pl.ds(h * pack, pack), :], src.at[h], load_sem.at[1 + h]) for h in range(2)
    ]
    load_tgt = [
        pltpu.make_async_copy(tgt_hbm.at[:, pl.ds(h * pack, pack), :], tgt.at[h], load_sem.at[3 + h]) for h in range(2)
    ]
    load_near = pltpu.make_async_copy(near_hbm, near, load_sem.at[5])
    load_ints = [
        pltpu.make_async_copy(a, b, load_sem.at[6 + i])
        for i, (a, b) in enumerate(
            ((off_hbm, off_ref), (cnt_hbm, cnt_ref), (fsrc_hbm, fsrc_ref), (fcnt_hbm, fcnt_ref))
        )
    ]
    for load in [*load_ints, *load_src]:
        load.start()

    def base(group):
        return jnp.where(core == 1, leaves - (group + 1) * size, group * size)

    def columns(group):
        return pl.ds(pl.multiple_of(base(group) * leaf, size * leaf), size * leaf)

    def taken(ref, sem):
        pltpu.make_async_copy(ref, ref, sem).wait()

    def inner_copy(k, group):
        own = mains[k % 2]
        return pltpu.make_async_remote_copy(
            src_ref=own.at[pl.ds(base(group), size)],
            dst_ref=own.at[pl.ds(leaves + base(group), size)],
            send_sem=in_send.at[k % 2],
            recv_sem=in_recv.at[k % 2],
            device_id=(inner,),
            device_id_type=MESH,
        )

    def outer_copy(k, place):
        buffer = next(b for b, places in enumerate(BUFFERS) if place in places)
        return pltpu.make_async_remote_copy(
            src_ref=mains[k % 2].at[pl.ds(base(SEND[place]), size)],
            dst_ref=exts[k % 2][buffer].at[pl.ds(BUFFERS[buffer].index(place) * size, size)],
            send_sem=ext_send.at[k % 2],
            recv_sem=ext_recv.at[k % 2, place],
            device_id=(outer,),
            device_id_type=MESH,
        )

    def far_copy(k, d):
        peer = lax.rem(me + d, n)
        return pltpu.make_async_remote_copy(
            src_ref=outgs[k % 2].at[peer],
            dst_ref=recvs[k % 2].at[me],
            send_sem=far_send.at[k % 2],
            recv_sem=far_recv.at[k % 2],
            device_id=(peer,),
            device_id_type=MESH,
        )

    blank = jnp.zeros((excite, leaf), jnp.bfloat16)
    for buffers in (mains, *exts):
        for buffer in buffers:
            buffer[buffer.shape[0] - 1] = blank
    for recv in recvs:
        recv[n] = jnp.zeros((pack, 2 * excite), jnp.bfloat16)
        recv[me] = jnp.zeros((pack, 2 * excite), jnp.bfloat16)
    cbuf[far_slots] = jnp.zeros((pack, 2 * excite), jnp.bfloat16)

    load_field.wait()
    for i in range(leaves):
        main_a[i] = field[:, i * leaf : (i + 1) * leaf]
    for load in [load_near, *load_tgt]:
        load.start()
    pl.semaphore_wait(barrier, n - 1)
    for place in (0, 1):
        outer_copy(0, place).start()
    for group in range(GROUPS):
        inner_copy(0, group).start()

    for load in load_ints:
        load.wait()

    def count(t, before):
        mine = 0
        live = fcnt_ref[t]
        for j in range(far_slots):
            mine += jnp.logical_and(fsrc_ref[j, t] == me, j < live).astype(jnp.int32)
        send_tab[t] = jnp.where(mine > 0, before, far_slots)
        return before + mine

    lax.fori_loop(0, n, count, jnp.int32(0))
    my_live = fcnt_ref[me]
    for j in range(far_slots):
        recv_tab[j] = jnp.where(j < my_live, fsrc_ref[j, me], n)

    def near_table():
        @pl.loop(0, leaves)
        def _(i):
            for j in range(slots):
                at = i + off_ref[j, i]
                live = j < cnt_ref[i]
                low, high = at < 0, at >= leaves
                far_side = jnp.where(core == 1, high.astype(jnp.int32), low.astype(jnp.int32)) == 1
                spot = jnp.where(low, at + leaves, jnp.where(high, at - leaves, at))
                own = jnp.logical_not(jnp.logical_or(low, high))
                near_side = jnp.where(own, spot, leaves + spot)
                use = jnp.logical_and(live, jnp.logical_not(far_side))
                near_tab[i * slots + j] = jnp.where(use, near_side, 2 * leaves)
                use = jnp.logical_and(live, far_side)
                for b, places in enumerate(BUFFERS):
                    found = len(places) * size
                    for order, place in enumerate(places):
                        group = SEND[place]
                        first = jnp.where(core == 1, group * size, leaves - (group + 1) * size)
                        inside = jnp.logical_and(spot >= first, spot < first + size)
                        inside = jnp.logical_and(inside, use)
                        found = jnp.where(inside, order * size + spot - first, found)
                    near_tab[((b + 1) * leaves + i) * slots + j] = found

    def project(group, fresh):
        cols = columns(group)
        charges = field[:, cols]
        for h in range(2):
            part = lax.dot_general(
                src[h, :, :, cols].reshape(half, size * leaf), charges, NT, preferred_element_type=jnp.float32
            )
            acc[h] = part if fresh else acc[h] + part

    def send_far(k):
        both = jnp.concatenate([acc[0], acc[1]], axis=1)
        cbuf[:far_slots] = both.reshape(far_slots, pack, 2 * excite).astype(jnp.bfloat16)
        outg = outgs[k % 2]

        @pl.loop(0, n // 2)
        def _(t):
            for u in range(2):
                outg[2 * t + u] = cbuf[send_tab[2 * t + u]]

        far_copy(k, n - 1).start()

        @pl.loop(1, n // 2)
        def _(d):
            for u in range(2):
                far_copy(k, n - 2 * d - u).start()

    def near_sum(k, group):
        own, ext = mains[k % 2], exts[k % 2][: NEED[group] + 1]
        sums = []
        for u in range(size):
            i = base(group) + u
            total = None
            for j in range(slots):
                x = own[near_tab[i * slots + j]]
                for b, buffer in enumerate(ext):
                    x += buffer[near_tab[((b + 1) * leaves + i) * slots + j]]
                part = jnp.dot(x, near[i, j], preferred_element_type=jnp.float32)
                total = part if total is None else total + part
            sums.append(total)
        return jnp.concatenate(sums, axis=1)

    def far_sum(coef, group):
        rows = tgt[:, :, :, columns(group)].reshape(2 * half, size * leaf)
        return jnp.dot(coef, rows, preferred_element_type=jnp.float32)

    def finish(k, group, total):
        cols = columns(group)
        out[k, :, cols] = total
        if k < last:
            rounded = total.astype(jnp.bfloat16)
            field[:, cols] = rounded
            for u in range(size):
                mains[(k + 1) % 2][base(group) + u] = rounded[:, u * leaf : (u + 1) * leaf]
            inner_copy(k + 1, group).start()
            if group in SEND[:2]:
                outer_copy(k + 1, SEND.index(group)).start()

    def wait_sent(k):
        own = mains[k % 2].at[pl.ds(0, leaves)]
        taken(own, ext_send.at[k % 2])
        taken(own, in_send.at[k % 2])

    for load in load_src:
        load.wait()
    for group in range(GROUPS):
        project(group, group == 0)

    for k in range(ITERS):
        part = {}

        def add_near(group):
            part[group] = True
            cols = columns(group)
            total = near_sum(k, group)
            if group in far_done:
                finish(k, group, total + out[k, :, cols])
            else:
                out[k, :, cols] = total

        def add_far(coef, group):
            far_done.add(group)
            cols = columns(group)
            total = far_sum(coef, group)
            if group in part:
                finish(k, group, total + out[k, :, cols])
            else:
                out[k, :, cols] = total

        far_done = set()
        send_far(k)
        outer_copy(k, 2).start()
        outer_copy(k, 3).start()
        if k == 0:
            near_table()
            load_near.wait()

            @pl.loop(0, leaves)
            def _(i):
                for j in range(slots):
                    near[i, j] = near[i, j].T

        taken(mains[k % 2].at[pl.ds(0, leaves)], in_recv.at[k % 2])
        for place in (0, 1):
            outer_copy(k, place).wait_recv()
        add_near(3)
        add_near(2)
        outer_copy(k, 2).wait_recv()
        add_near(1)

        whole = recvs[k % 2].at[pl.ds(0, n - 1)]
        taken(whole, far_send.at[k % 2])
        taken(whole, far_recv.at[k % 2])

        got = jnp.concatenate([recvs[k % 2][recv_tab[j]] for j in range(far_slots)], axis=0)
        got = got.astype(jnp.float32).T.astype(jnp.bfloat16)
        coef = jnp.concatenate([got[:excite], got[excite:]], axis=1)
        if k == 0:
            for load in load_tgt:
                load.wait()
        if 1 <= k < last:
            wait_sent(k - 1)
        if k < last:
            add_far(coef, 1)
            add_far(coef, 0)
            add_far(coef, 3)
            add_far(coef, 2)
            outer_copy(k, 3).wait_recv()
            add_near(0)
            for at, group in enumerate((1, 3, 2, 0)):
                project(group, at == 0)
        else:
            for group in (3, 2, 1, 0):
                add_far(coef, group)
            outer_copy(k, 3).wait_recv()
            add_near(0)
    for k in range(max(ITERS - 2, 0), ITERS):
        wait_sent(k)


def shards(n, excitation, near_tiles, near_offset, near_count, far_src, far_count, source_factor, target_factor):
    excite, panels = excitation.shape
    leaves, slots, leaf, _ = near_tiles.shape
    far_slots, rank, _ = source_factor.shape
    size, pack = leaves // GROUPS, rank // 2
    bf, f32 = jnp.bfloat16, jnp.float32
    hbm = pl.BlockSpec(memory_space=pltpu.HBM)
    ext = [pltpu.VMEM((len(places) * size + 1, excite, leaf), bf) for places in BUFFERS]
    return pl.pallas_call(
        functools.partial(kernel, n),
        out_shape=pltpu.VMEM((ITERS, excite, panels), f32),
        in_specs=[hbm] * 8,
        out_specs=pl.BlockSpec(memory_space=pltpu.VMEM),
        scratch_shapes=[
            pltpu.SMEM((slots, leaves), jnp.int32),
            pltpu.SMEM((leaves,), jnp.int32),
            pltpu.SMEM((far_slots, n), jnp.int32),
            pltpu.SMEM((n,), jnp.int32),
            pltpu.VMEM((leaves, slots, leaf, leaf), bf),
            pltpu.VMEM((2, far_slots, pack, panels), bf),
            pltpu.VMEM((2, far_slots, pack, panels), bf),
            pltpu.VMEM((excite, panels), bf),
            pltpu.VMEM((2 * leaves + 1, excite, leaf), bf),
            pltpu.VMEM((2 * leaves + 1, excite, leaf), bf),
            *ext,
            *ext,
            pltpu.VMEM((n + 1, pack, 2 * excite), bf),
            pltpu.VMEM((n + 1, pack, 2 * excite), bf),
            pltpu.VMEM((n, pack, 2 * excite), bf),
            pltpu.VMEM((n, pack, 2 * excite), bf),
            pltpu.VMEM((far_slots + 1, pack, 2 * excite), bf),
            pltpu.VMEM((2, far_slots * pack, excite), f32),
            pltpu.SMEM(((1 + len(BUFFERS)) * leaves * slots,), jnp.int32),
            pltpu.SMEM((n,), jnp.int32),
            pltpu.SMEM((far_slots,), jnp.int32),
            pltpu.SemaphoreType.DMA((10,)),
            pltpu.SemaphoreType.DMA((2,)),
            pltpu.SemaphoreType.DMA((2,)),
            pltpu.SemaphoreType.DMA((2,)),
            pltpu.SemaphoreType.DMA((2, GROUPS)),
            pltpu.SemaphoreType.DMA((2,)),
            pltpu.SemaphoreType.DMA((2,)),
        ],
        compiler_params=pltpu.CompilerParams(
            collective_id=0, has_side_effects=True, vmem_limit_bytes=54 * 1024 * 1024
        ),
    )(near_offset.T, near_count, far_src.T, far_count, excitation, near_tiles, source_factor, target_factor)


def solution(mesh):
    in_specs = (
        P(None, "panels"),
        P("panels", None, None, None),
        P("panels", None),
        P("panels"),
        P(),
        P(),
        P(None, None, "panels"),
        P(None, None, "panels"),
    )
    return jax.shard_map(
        functools.partial(shards, mesh.shape["panels"]),
        mesh=mesh,
        in_specs=in_specs,
        out_specs=P(None, None, "panels"),
        check_vma=False,
    )
```
